32 devices in a mesh: groups: 2 (over x), tile: 16 (over z, y, core).
Axes of the slice: x: 2, y: 2, z: 4, core: 2. Of those that a mesh axis runs over, the one named last changes fastest.
Arguments:
- echoes: float32 [2, 32, 16384], P(None, ('groups', 'tile')), parts along dimension 1, may hold values from -6 to 6
- bin_start: int32 [32, 16], P(('groups', 'tile')), parts along dimension 0, may hold values from 0 to 16128
- bin_fraction: float32 [16, 32], P(None, ('groups', 'tile')), parts along dimension 1, may hold values from 0 to 1
- row_phase: float32 [16, 32, 128], P(None, ('groups', 'tile')), parts along dimension 1, may hold values from -3.140625 to 3.140625
- column_phase: float32 [16, 32, 128], P(None, ('groups', 'tile')), parts along dimension 1, may hold values from -3.140625 to 3.140625
- row_bin: int32 [16, 32, 128], P(None, ('groups', 'tile')), parts along dimension 1, may hold values from 0 to 127
- column_bin: int32 [16, 32, 128], P(None, ('groups', 'tile')), parts along dimension 1, may hold values from 0 to 127
Outputs:
- focused: float32 [2, 32, 128, 128], P(None, ('groups', 'tile')), parts along dimension 1
- correction: float32 [2, 32], P(None, ('groups', 'tile')), parts along dimension 1
The draws below stay inside these ranges and needn't reach their ends.
There are 2 independent parts, one for each index of `groups`. The reference program is written for one: setup_inputs(seed, part) draws one part's arguments, and reference() takes and returns one part's arrays. A program takes and returns all parts, laid end to end along the dimension named above; each array names one. Nothing has to cross between parts.
Inputs may be any that keep to these rules, and one draw needn't show every extreme that they name: The window of 256 range bins that begins at bin_start lies within the 16384 bins.
All inputs are finite; a program needn't handle non-finite values.
Results may differ from the reference program's by a relative error of at most 0.012.
Values may be sent and summed in bfloat16 or wider, within the bound.
A program may use at most 320 MiB of HBM per device.

```python
import math
import jax
import jax.numpy as jnp
from jax import lax

SAMPLES = 16384
ROWS = 128
COLS = 128
BINR = 128
BINC = 128
PULSES = 16
TILES = 16


def plant(result, own_key, low, high):
    longest = result.shape.index(max(result.shape))
    spots = []
    for shift in (0, 1):
        where = [jax.random.randint(jax.random.fold_in(own_key, axis), (), 0, length) for axis, length in enumerate(result.shape)]
        where[longest] = (where[longest] + shift) % result.shape[longest]
        spots.append(tuple(where))
    return result.at[spots[0]].set(low).at[spots[1]].set(high)


def block_levels(key, dims, pieces, low, high):
    factor_of = 1.0
    for dim, parts in pieces:
        draws = jax.random.uniform(jax.random.fold_in(jax.random.fold_in(key, 6), dim), (parts,), jnp.float32, low / len(pieces), high / len(pieces))
        factor_of = factor_of * jnp.repeat(jnp.exp(draws), dims[dim] // parts).reshape((-1,) + (1,) * (len(dims) - 1 - dim))
    return factor_of


def normal_values(stream_key, shape, scale, most, cuts=(), kind=jnp.bfloat16):
    array = scale * jax.random.normal(stream_key, shape, jnp.float32)
    if cuts:
        array = array * block_levels(stream_key, shape, cuts, -0.22, 0.18)
    return jnp.clip(array, -most, most).astype(kind)


def setup_inputs(seed: int = 0, part: int = 0) -> dict:
    keys = jax.random.split(jax.random.key(seed), 8)
    part_keys = jax.random.split(jax.random.fold_in(keys[7], part), 8)
    return {
        "echoes": normal_values(part_keys[0], (2, PULSES, SAMPLES), 1.0, 6.0, ((1, 16),), jnp.float32),
        "bin_start": plant(jax.random.randint(part_keys[1], (PULSES, TILES), 0, SAMPLES - BINR - BINC + 1), jax.random.fold_in(part_keys[1], 1), 0, SAMPLES - BINR - BINC).astype(jnp.int32),
        "bin_fraction": jnp.clip(1.0 * jax.random.uniform(part_keys[2], (PULSES, TILES), jnp.float32) ** block_levels(part_keys[2], (PULSES, TILES), ((1, 16),), -0.2, 0.2), 0.0, 1.0),
        "row_phase": jnp.clip(jax.random.uniform(part_keys[3], (PULSES, TILES, ROWS), jnp.float32, -3.140625, 3.140625), -3.140625, 3.140625),
        "column_phase": jnp.clip(jax.random.uniform(part_keys[4], (PULSES, TILES, COLS), jnp.float32, -3.140625, 3.140625), -3.140625, 3.140625),
        "row_bin": plant(jax.random.randint(part_keys[5], (PULSES, TILES, ROWS), 0, BINR), jax.random.fold_in(part_keys[5], 1), 0, BINR - 1).astype(jnp.int32),
        "column_bin": plant(jax.random.randint(part_keys[6], (PULSES, TILES, COLS), 0, BINC), jax.random.fold_in(part_keys[6], 1), 0, BINC - 1).astype(jnp.int32),
    }


def rounded(values):
    return lax.optimization_barrier(values.astype(jnp.bfloat16)).astype(jnp.float32)

def normalize(real_part, imag_part):
    magnitude = real_part * real_part + imag_part * imag_part
    denominator = jnp.sqrt(magnitude + jnp.mean(magnitude) + 1e-06)
    return (real_part / denominator, imag_part / denominator)

def reference(echoes, bin_start, bin_fraction, row_phase, column_phase, row_bin, column_bin):
    signal = echoes[0] + 1j * echoes[1]
    spectrum = jnp.fft.fft(signal, axis=1) / math.sqrt(SAMPLES)
    spectra = rounded(jnp.stack([jnp.real(spectrum), jnp.imag(spectrum)]))
    window_len = BINR + BINC
    offsets = jnp.arange(window_len, dtype=jnp.int32)
    shifts = jnp.arange(BINC, dtype=jnp.int32)
    norm_scale = 1.0 / math.sqrt(PULSES)
    pulse_ids = jnp.arange(PULSES, dtype=jnp.int32)

    def contribution(pulse_id):
        begins = bin_start[pulse_id][:, None] + offsets[None, :]
        window = spectra[:, pulse_id][:, begins]
        weight_frac = bin_fraction[pulse_id][None, :, None]
        profile = rounded((1.0 - weight_frac) * window[..., :-1] + weight_frac * window[..., 1:])
        index_rows = (row_bin[pulse_id][:, :, None] + shifts[None, None, :]).reshape(TILES, ROWS * BINC)
        chosen_real = jnp.take_along_axis(profile[0], index_rows, axis=1).reshape(TILES, ROWS, BINC)
        chosen_imag = jnp.take_along_axis(profile[1], index_rows, axis=1).reshape(TILES, ROWS, BINC)
        row_cosine = rounded(jnp.cos(row_phase[pulse_id]))[:, :, None]
        row_sine = rounded(jnp.sin(row_phase[pulse_id]))[:, :, None]
        steer_real = rounded(row_cosine * chosen_real - row_sine * chosen_imag)
        steer_imag = rounded(row_cosine * chosen_imag + row_sine * chosen_real)
        index_columns = jnp.broadcast_to(column_bin[pulse_id][:, None, :], (TILES, ROWS, COLS))
        moved_real = jnp.take_along_axis(steer_real, index_columns, axis=2)
        moved_imag = jnp.take_along_axis(steer_imag, index_columns, axis=2)
        column_cosine = rounded(jnp.cos(column_phase[pulse_id]))[:, None, :]
        column_sine = rounded(jnp.sin(column_phase[pulse_id]))[:, None, :]
        return (column_cosine * moved_real - column_sine * moved_imag, column_cosine * moved_imag + column_sine * moved_real)

    def image_of(weight_real, weight_imag):

        def visit_pulse(running, pulse_id):
            part_real, part_imag = contribution(pulse_id)
            new_real = running[0] + weight_real[pulse_id] * part_real - weight_imag[pulse_id] * part_imag
            new_imag = running[1] + weight_real[pulse_id] * part_imag + weight_imag[pulse_id] * part_real
            return ((new_real, new_imag), None)
        zero_image = jnp.zeros((TILES, ROWS, COLS), jnp.float32)
        (image_real, image_imag), _ = lax.scan(visit_pulse, (zero_image, zero_image), pulse_ids)
        return (image_real * norm_scale, image_imag * norm_scale)

    def correlate(image_real, image_imag):

        def visit_pulse(running, pulse_id):
            part_real, part_imag = contribution(pulse_id)
            totals = (jnp.sum(part_real * image_real + part_imag * image_imag), jnp.sum(part_real * image_imag - part_imag * image_real), jnp.sum(part_real * part_real + part_imag * part_imag))
            return (running, totals)
        _, totals = lax.scan(visit_pulse, jnp.zeros((), jnp.float32), pulse_ids)
        return totals
    unit_weights = jnp.ones((PULSES,), jnp.float32)
    zero_weights = jnp.zeros((PULSES,), jnp.float32)
    first_real, first_imag = image_of(unit_weights, zero_weights)
    cross_real, cross_imag, energy = correlate(first_real, first_imag)
    one_real, one_imag = normalize(cross_real - energy * norm_scale, cross_imag)
    second_real, second_imag = image_of(one_real, one_imag)
    cross_real, cross_imag, _ = correlate(second_real, second_imag)
    rest_real = cross_real - one_real * energy * norm_scale
    rest_imag = cross_imag - one_imag * energy * norm_scale
    again_real = one_real * rest_real + one_imag * rest_imag
    again_imag = one_real * rest_imag - one_imag * rest_real
    two_real, two_imag = normalize(again_real, again_imag)
    total_real = one_real * two_real - one_imag * two_imag
    total_imag = one_real * two_imag + one_imag * two_real
    final_real, final_imag = image_of(total_real, total_imag)
    return (jnp.stack([final_real, final_imag]), jnp.stack([total_real, total_imag]))
```

```python
import functools
import math

import jax
import jax.numpy as jnp
import numpy as np
from jax import lax
from jax.experimental import pallas as pl
from jax.experimental.pallas import tpu as pltpu
from jax.sharding import PartitionSpec as P

LANES = 128
OCTET = 8
MESH = pl.DeviceIdType.MESH
F32 = jnp.float32
BF16 = jnp.bfloat16


def tables(samples):
    inner = LANES
    outer = samples // inner

    def wave(rows, columns, period):
        product = np.arange(rows)[:, None] * np.arange(columns)[None, :] % period
        phases = product * (2.0 * np.pi / period)
        return np.cos(phases), np.sin(phases)

    def split(table):
        table = table.astype(np.float32)
        high = table.astype(jnp.bfloat16)
        low = (table - high.astype(np.float32)).astype(jnp.bfloat16)
        return np.stack([high, low])

    first = split(np.concatenate(wave(outer, outer, outer), 1))
    last = split(np.concatenate(wave(inner, inner, inner), 1))
    turn = np.stack(wave(outer, inner, samples)) / math.sqrt(samples)
    return first, turn.astype(np.float32), last


def fold_table(pulses):
    block = np.arange(pulses * 2 * OCTET) // OCTET
    pulse, part = block // 2, block % 2
    lane = np.arange(LANES)
    same = [(lane[None, :] == pulse[:, None] + shift * pulses) for shift in (0, 1)]
    real_in = part[:, None] == 0
    real_rows = (same[0] & real_in) * 1.0 + (same[1] & ~real_in) * 1.0
    imag_rows = (same[0] & ~real_in) * 1.0 - (same[1] & real_in) * 1.0
    return np.stack([real_rows, imag_rows]).astype(np.float32)


def dot(a, b, dims=((1,), (0,)), precision=None):
    return lax.dot_general(a, b, (dims, ((), ())), precision=precision, preferred_element_type=F32)


def split3(table_ref, data, dims):
    high = data.astype(BF16)
    low = (data - high.astype(F32)).astype(BF16)
    return dot(table_ref[0], high, dims) + (dot(table_ref[1], high, dims) + dot(table_ref[0], low, dims))


def normalize(real_part, imag_part, axis, count):
    magnitude = real_part * real_part + imag_part * imag_part
    mean = jnp.sum(magnitude, axis=axis, keepdims=True) / count
    denominator = jnp.sqrt(magnitude + mean + 1e-06)
    return real_part / denominator, imag_part / denominator


def kernel(
    n, starts, echo, fraction, row_phase, column_phase, row_bin, column_bin, first, turn, last, fold,
    focused, correction,
    spec, outgoing, gathered, steer, parts, gram_in, message, messages, weights,
    send_sem, recv_sem, send_sem2, recv_sem2,
):
    me = lax.axis_index("tile")
    rows = row_phase.shape[2]
    scale = 1.0 / math.sqrt(n)

    barrier = pltpu.get_barrier_semaphore()
    for k in range(1, n):
        pl.semaphore_signal(barrier, inc=1, device_id={"tile": lax.rem(me + k, n)}, device_id_type=MESH)

    real, imag = echo[0], echo[1]
    data = jnp.concatenate(
        [jnp.concatenate([real, imag], 1), jnp.concatenate([imag, -real], 1)], 0
    )
    section = split3(first, data, ((1,), (0,)))
    half = section.shape[1] // 2
    real, imag = section[:, :half], section[:, half:]
    turned_real = real * turn[0] + imag * turn[1]
    turned_imag = imag * turn[0] - real * turn[1]
    data = jnp.concatenate(
        [jnp.concatenate([turned_real, turned_imag], 1), jnp.concatenate([turned_imag, -turned_real], 1)], 0
    )
    spectrum = split3(last, data, ((1,), (1,)))
    bins = spectrum.shape[0]
    spectrum = spectrum.astype(BF16).astype(F32)
    for h in range(2):
        spec[h, 0:bins, :] = spectrum[:, h * LANES : (h + 1) * LANES]
        spec[h, bins:, :] = jnp.zeros((spec.shape[1] - bins, LANES), F32)

    lane = lax.broadcasted_iota(jnp.int32, (OCTET, LANES), 1)
    for t in range(n):
        start = starts[0, t]
        top = start // LANES
        left = LANES - start % LANES
        pieces = []
        for h in range(2):
            moved = pltpu.roll(spec[h, pl.ds(top, OCTET), :], left % LANES, 1)
            below = pltpu.roll(moved, OCTET - 1, 0)
            pieces.append(jnp.where(lane < left, moved, below)[0:2])
        outgoing[t] = jnp.concatenate(pieces, 0).astype(BF16)

    pl.semaphore_wait(barrier, n - 1)

    def window_copy(k):
        target = lax.rem(me + k, n)
        return pltpu.make_async_remote_copy(
            src_ref=outgoing.at[target],
            dst_ref=gathered.at[me],
            send_sem=send_sem.at[k],
            recv_sem=recv_sem.at[k],
            device_id={"tile": target},
            device_id_type=MESH,
        )

    copies = [window_copy(k) for k in range(1, n)]
    for copy in copies:
        copy.start()
    gathered[me] = outgoing[me]

    def rounded(values):
        return values.astype(BF16).astype(F32)

    angles = row_phase[:, 0, :]
    left_side = jnp.concatenate(
        [
            rounded(jnp.cos(angles)),
            rounded(jnp.sin(angles)),
            row_bin[:, 0, :].astype(F32),
            jnp.ones((n, rows), F32),
        ],
        0,
    )
    left_side = left_side.T.astype(BF16)
    angles = column_phase[:, 0, :]
    cosine, sine = rounded(jnp.cos(angles)), rounded(jnp.sin(angles))
    zero, one = jnp.zeros((n, LANES), F32), jnp.ones((n, LANES), F32)
    right_side = jnp.concatenate(
        [
            jnp.concatenate([cosine, sine, zero], 1),
            jnp.concatenate([-sine, cosine, zero], 1),
            jnp.concatenate([zero, zero, one], 1),
            jnp.concatenate([zero, zero, column_bin[:, 0, :].astype(F32)], 1),
        ],
        0,
    )
    owner = lax.rem(lax.broadcasted_iota(jnp.int32, right_side.shape, 0), n)
    for p in range(n):
        steer[p] = dot(left_side, jnp.where(owner == p, right_side, 0.0).astype(BF16))

    for copy in copies:
        copy.wait()

    lane4 = lax.broadcasted_iota(jnp.int32, (4, LANES), 1)
    for p in range(n):
        window = gathered[p].astype(F32)
        moved = pltpu.roll(window, LANES - 1, 1)
        below = jnp.concatenate([moved[1:4], moved[0:1]], 0)
        shifted = jnp.where(lane4 == LANES - 1, below, moved)
        share = fraction[p : p + 1, 0:1]
        profile = ((1.0 - share) * window + share * shifted).astype(BF16).astype(F32)
        index = steer[p, :, 2 * LANES :].astype(jnp.int32)
        low = index < LANES
        index = index & (LANES - 1)

        def pick(row):
            source = jnp.broadcast_to(profile[row : row + 1, :], (rows, LANES))
            return jnp.take_along_axis(source, index, axis=1, mode="promise_in_bounds")

        real = jnp.where(low, pick(0), pick(1))
        imag = jnp.where(low, pick(2), pick(3))
        turn_real, turn_imag = steer[p, :, :LANES], steer[p, :, LANES : 2 * LANES]
        part_real = turn_real * real - turn_imag * imag
        part_imag = turn_real * imag + turn_imag * real
        parts[p, 0] = part_real
        parts[p, 1] = part_imag
        for t in range(rows // OCTET):
            pair = jnp.concatenate(
                [part_real[t * OCTET : (t + 1) * OCTET], part_imag[t * OCTET : (t + 1) * OCTET]], 0
            )
            gram_in[p * 2 * OCTET : (p + 1) * 2 * OCTET, t * LANES : (t + 1) * LANES] = pair.astype(BF16)

    values = gram_in[...]
    product = dot(values, values, ((1,), (1,)))
    row_id = lax.broadcasted_iota(jnp.int32, product.shape, 0)
    column_id = lax.broadcasted_iota(jnp.int32, product.shape, 1)
    product = jnp.where(lax.rem(row_id, OCTET) == lax.rem(column_id, OCTET), product, 0.0)
    product = product.reshape(n, 2, OCTET, product.shape[1])
    gram = dot(jnp.sum(product[:, 0], axis=1), fold[0], precision=lax.Precision.HIGHEST)
    gram = gram + dot(jnp.sum(product[:, 1], axis=1), fold[1], precision=lax.Precision.HIGHEST)
    groups = LANES // (2 * n)
    depth = n // groups
    packed = gram[0:depth]
    for g in range(1, groups):
        packed = packed + pltpu.roll(gram[g * depth : (g + 1) * depth], g * 2 * n, 1)
    message[...] = packed
    messages[me] = packed

    def gram_copy(k):
        return pltpu.make_async_remote_copy(
            src_ref=message,
            dst_ref=messages.at[me],
            send_sem=send_sem2.at[k],
            recv_sem=recv_sem2.at[k],
            device_id={"tile": lax.rem(me + k, n)},
            device_id_type=MESH,
        )

    copies = [gram_copy(k) for k in range(1, n)]
    for copy in copies:
        copy.start()
    for copy in copies:
        copy.wait()

    total = jnp.sum(messages[...], axis=0)
    gram = jnp.concatenate(
        [total] + [pltpu.roll(total, LANES - g * 2 * n, 1) for g in range(1, groups)], 0
    )
    row_id = lax.broadcasted_iota(jnp.int32, gram.shape, 0)
    column_id = lax.broadcasted_iota(jnp.int32, gram.shape, 1)
    off_diagonal = (column_id < n) & (column_id != row_id)
    gram_real = jnp.where(off_diagonal, gram * scale, 0.0)
    gram_imag = jnp.where(off_diagonal, pltpu.roll(gram, LANES - n, 1) * scale, 0.0)

    def along(values, axis):
        return jnp.sum(values, axis=axis, keepdims=True)

    one_real, one_imag = normalize(along(gram_real, 1), along(gram_imag, 1), 0, n)
    row_real, row_imag = normalize(along(gram_real, 0), -along(gram_imag, 0), 1, n)
    rest_real = along(gram_real * row_real - gram_imag * row_imag, 1)
    rest_imag = along(gram_real * row_imag + gram_imag * row_real, 1)
    again_real = one_real * rest_real + one_imag * rest_imag
    again_imag = one_real * rest_imag - one_imag * rest_real
    two_real, two_imag = normalize(again_real, again_imag, 0, n)
    total_real = one_real * two_real - one_imag * two_imag
    total_imag = one_real * two_imag + one_imag * two_real
    mine = lax.broadcasted_iota(jnp.int32, total_real.shape, 0) == me
    correction[0:1, :] = along(jnp.where(mine, total_real, 0.0), 0)
    correction[1:2, :] = along(jnp.where(mine, total_imag, 0.0), 0)
    weights[0] = jnp.broadcast_to(total_real * scale, (n, LANES))
    weights[1] = jnp.broadcast_to(total_imag * scale, (n, LANES))

    step = 4 * OCTET
    for t in range(rows // step):
        span = slice(t * step, (t + 1) * step)
        sum_real = jnp.zeros((step, LANES), F32)
        sum_imag = jnp.zeros((step, LANES), F32)
        for p in range(n):
            weight_real = weights[0, p : p + 1, :]
            weight_imag = weights[1, p : p + 1, :]
            part_real, part_imag = parts[p, 0, span, :], parts[p, 1, span, :]
            sum_real = sum_real + (weight_real * part_real - weight_imag * part_imag)
            sum_imag = sum_imag + (weight_real * part_imag + weight_imag * part_real)
        focused[0, 0, span, :] = sum_real
        focused[1, 0, span, :] = sum_imag


def solution(mesh):
    n = mesh.shape["tile"]

    def per_device(echoes, bin_start, bin_fraction, row_phase, column_phase, row_bin, column_bin):
        samples = echoes.shape[2]
        rows, columns = row_phase.shape[2], column_phase.shape[2]
        first, turn, last = tables(samples)
        bins = samples // LANES
        echo = echoes.reshape(2, bins, LANES)
        fold = fold_table(n)
        vmem = pl.BlockSpec(memory_space=pltpu.VMEM)
        depth = n * 2 * n // LANES
        return pl.pallas_call(
            functools.partial(kernel, n),
            out_shape=(
                jax.ShapeDtypeStruct((2, 1, rows, columns), F32),
                jax.ShapeDtypeStruct((2, 1), F32),
            ),
            in_specs=[pl.BlockSpec(memory_space=pltpu.SMEM)] + [vmem] * 10,
            out_specs=(vmem, vmem),
            scratch_shapes=[
                pltpu.VMEM((2, bins + OCTET, LANES), F32),
                pltpu.VMEM((n, 4, LANES), BF16),
                pltpu.VMEM((n, 4, LANES), BF16),
                pltpu.VMEM((n, rows, 3 * LANES), F32),
                pltpu.VMEM((n, 2, rows, columns), F32),
                pltpu.VMEM((n * 2 * OCTET, rows // OCTET * columns), BF16),
                pltpu.VMEM((depth, LANES), F32),
                pltpu.VMEM((n, depth, LANES), F32),
                pltpu.VMEM((2, n, LANES), F32),
                pltpu.SemaphoreType.DMA((n,)),
                pltpu.SemaphoreType.DMA((n,)),
                pltpu.SemaphoreType.DMA((n,)),
                pltpu.SemaphoreType.DMA((n,)),
            ],
            compiler_params=pltpu.CompilerParams(collective_id=0, has_side_effects=True),
        )(
            bin_start, echo, bin_fraction, row_phase, column_phase, row_bin, column_bin,
            jnp.asarray(first), jnp.asarray(turn), jnp.asarray(last), jnp.asarray(fold),
        )

    split = ("groups", "tile")
    in_specs = (
        P(None, split, None),
        P(split, None),
        P(None, split),
        P(None, split, None),
        P(None, split, None),
        P(None, split, None),
        P(None, split, None),
    )
    out_specs = (P(None, split, None, None), P(None, split))
    return jax.shard_map(per_device, mesh=mesh, in_specs=in_specs, out_specs=out_specs, check_vma=False)
```

```python
import functools
import math

import jax
import jax.numpy as jnp
import numpy as np
from jax import lax
from jax.experimental import pallas as pl
from jax.experimental.pallas import tpu as pltpu
from jax.sharding import PartitionSpec as P

LANES = 128
OCTET = 8
MESH = pl.DeviceIdType.MESH
F32 = jnp.float32
BF16 = jnp.bfloat16


def tables(samples):
    inner = LANES
    outer = samples // inner

    def wave(rows, columns, period):
        product = np.arange(rows)[:, None] * np.arange(columns)[None, :] % period
        phases = product * (2.0 * np.pi / period)
        return np.cos(phases), np.sin(phases)

    def split(table):
        table = table.astype(np.float32)
        high = table.astype(jnp.bfloat16)
        low = (table - high.astype(np.float32)).astype(jnp.bfloat16)
        return np.stack([high, low])

    first = split(np.concatenate(wave(outer, outer, outer), 1))
    last = split(np.concatenate(wave(inner, inner, inner), 1))
    turn = np.stack(wave(outer, inner, samples)) / math.sqrt(samples)
    return first, turn.astype(np.float32), last


def fold_table(pulses):
    block = np.arange(pulses * 2 * OCTET) // OCTET
    pulse, part = block // 2, block % 2
    lane = np.arange(LANES)
    same = [(lane[None, :] == pulse[:, None] + shift * pulses) for shift in (0, 1)]
    real_in = part[:, None] == 0
    real_rows = (same[0] & real_in) * 1.0 + (same[1] & ~real_in) * 1.0
    imag_rows = (same[0] & ~real_in) * 1.0 - (same[1] & real_in) * 1.0
    return np.stack([real_rows, imag_rows]).astype(np.float32)


def dot(a, b, dims=((1,), (0,)), precision=None):
    return lax.dot_general(a, b, (dims, ((), ())), precision=precision, preferred_element_type=F32)


def split3(table_ref, data, dims):
    high = data.astype(BF16)
    low = (data - high.astype(F32)).astype(BF16)
    return dot(table_ref[0], high, dims) + (dot(table_ref[1], high, dims) + dot(table_ref[0], low, dims))


def normalize(real_part, imag_part, axis, count):
    magnitude = real_part * real_part + imag_part * imag_part
    mean = jnp.sum(magnitude, axis=axis, keepdims=True) / count
    denominator = jnp.sqrt(magnitude + mean + 1e-06)
    return real_part / denominator, imag_part / denominator


def kernel(
    n, starts, echo, fraction, row_phase, column_phase, row_bin, column_bin, first, turn, last, fold,
    focused, correction,
    spec, outgoing, gathered, steer, parts, gram_in, message, messages, weights,
    send_sem, recv_sem, send_sem2, recv_sem2,
):
    me = lax.axis_index("tile")
    rows = row_phase.shape[2]
    scale = 1.0 / math.sqrt(n)

    barrier = pltpu.get_barrier_semaphore()
    for k in range(1, n):
        pl.semaphore_signal(barrier, inc=1, device_id={"tile": lax.rem(me + k, n)}, device_id_type=MESH)

    real, imag = echo[0], echo[1]
    data = jnp.concatenate(
        [jnp.concatenate([real, imag], 1), jnp.concatenate([imag, -real], 1)], 0
    )
    section = split3(first, data, ((1,), (0,)))
    half = section.shape[1] // 2
    real, imag = section[:, :half], section[:, half:]
    turned_real = real * turn[0] + imag * turn[1]
    turned_imag = imag * turn[0] - real * turn[1]
    data = jnp.concatenate(
        [jnp.concatenate([turned_real, turned_imag], 1), jnp.concatenate([turned_imag, -turned_real], 1)], 0
    )
    spectrum = split3(last, data, ((1,), (1,)))
    bins = spectrum.shape[0]
    spectrum = spectrum.astype(BF16).astype(F32)
    for h in range(2):
        spec[h, 0:bins, :] = spectrum[:, h * LANES : (h + 1) * LANES]
        spec[h, bins:, :] = jnp.zeros((spec.shape[1] - bins, LANES), F32)

    lane = lax.broadcasted_iota(jnp.int32, (OCTET, LANES), 1)
    for t in range(n):
        start = starts[0, t]
        top = start // LANES
        left = LANES - start % LANES
        pieces = []
        for h in range(2):
            moved = pltpu.roll(spec[h, pl.ds(top, OCTET), :], left % LANES, 1)
            below = pltpu.roll(moved, OCTET - 1, 0)
            pieces.append(jnp.where(lane < left, moved, below)[0:2])
        outgoing[t] = jnp.concatenate(pieces, 0).astype(BF16)

    pl.semaphore_wait(barrier, n - 1)

    def window_copy(k):
        target = lax.rem(me + k, n)
        return pltpu.make_async_remote_copy(
            src_ref=outgoing.at[target],
            dst_ref=gathered.at[me],
            send_sem=send_sem.at[k],
            recv_sem=recv_sem.at[k],
            device_id={"tile": target},
            device_id_type=MESH,
        )

    copies = [window_copy(k) for k in range(1, n)]
    for copy in copies:
        copy.start()
    gathered[me] = outgoing[me]

    def rounded(values):
        return values.astype(BF16).astype(F32)

    angles = row_phase[:, 0, :]
    left_side = jnp.concatenate(
        [
            rounded(jnp.cos(angles)),
            rounded(jnp.sin(angles)),
            row_bin[:, 0, :].astype(F32),
            jnp.ones((n, rows), F32),
        ],
        0,
    )
    left_side = left_side.T.astype(BF16)
    angles = column_phase[:, 0, :]
    cosine, sine = rounded(jnp.cos(angles)), rounded(jnp.sin(angles))
    zero, one = jnp.zeros((n, LANES), F32), jnp.ones((n, LANES), F32)
    right_side = jnp.concatenate(
        [
            jnp.concatenate([cosine, sine, zero], 1),
            jnp.concatenate([-sine, cosine, zero], 1),
            jnp.concatenate([zero, zero, one], 1),
            jnp.concatenate([zero, zero, column_bin[:, 0, :].astype(F32)], 1),
        ],
        0,
    )
    owner = lax.rem(lax.broadcasted_iota(jnp.int32, right_side.shape, 0), n)
    for p in range(n):
        steer[p] = dot(left_side, jnp.where(owner == p, right_side, 0.0).astype(BF16))

    for copy in copies:
        copy.wait()

    lane4 = lax.broadcasted_iota(jnp.int32, (4, LANES), 1)
    for p in range(n):
        window = gathered[p].astype(F32)
        moved = pltpu.roll(window, LANES - 1, 1)
        below = jnp.concatenate([moved[1:4], moved[0:1]], 0)
        shifted = jnp.where(lane4 == LANES - 1, below, moved)
        share = fraction[0, p]
        profile = ((1.0 - share) * window + share * shifted).astype(BF16).astype(F32)
        index = steer[p, :, 2 * LANES :].astype(jnp.int32)
        low = index < LANES
        index = index & (LANES - 1)

        def pick(row):
            source = jnp.broadcast_to(profile[row : row + 1, :], (rows, LANES))
            return jnp.take_along_axis(source, index, axis=1, mode="promise_in_bounds")

        real = jnp.where(low, pick(0), pick(1))
        imag = jnp.where(low, pick(2), pick(3))
        turn_real, turn_imag = steer[p, :, :LANES], steer[p, :, LANES : 2 * LANES]
        part_real = turn_real * real - turn_imag * imag
        part_imag = turn_real * imag + turn_imag * real
        parts[p, 0] = part_real
        parts[p, 1] = part_imag
        for t in range(rows // OCTET):
            pair = jnp.concatenate(
                [part_real[t * OCTET : (t + 1) * OCTET], part_imag[t * OCTET : (t + 1) * OCTET]], 0
            )
            gram_in[p * 2 * OCTET : (p + 1) * 2 * OCTET, t * LANES : (t + 1) * LANES] = pair.astype(BF16)

    values = gram_in[...]
    product = dot(values, values, ((1,), (1,)))
    row_id = lax.broadcasted_iota(jnp.int32, product.shape, 0)
    column_id = lax.broadcasted_iota(jnp.int32, product.shape, 1)
    product = jnp.where(lax.rem(row_id, OCTET) == lax.rem(column_id, OCTET), product, 0.0)
    product = product.reshape(n, 2, OCTET, product.shape[1])
    gram = dot(jnp.sum(product[:, 0], axis=1), fold[0], precision=lax.Precision.HIGHEST)
    gram = gram + dot(jnp.sum(product[:, 1], axis=1), fold[1], precision=lax.Precision.HIGHEST)
    groups = LANES // (2 * n)
    depth = n // groups
    packed = gram[0:depth]
    for g in range(1, groups):
        packed = packed + pltpu.roll(gram[g * depth : (g + 1) * depth], g * 2 * n, 1)
    message[...] = packed
    messages[me] = packed

    def gram_copy(k):
        return pltpu.make_async_remote_copy(
            src_ref=message,
            dst_ref=messages.at[me],
            send_sem=send_sem2.at[k],
            recv_sem=recv_sem2.at[k],
            device_id={"tile": lax.rem(me + k, n)},
            device_id_type=MESH,
        )

    copies = [gram_copy(k) for k in range(1, n)]
    for copy in copies:
        copy.start()
    for copy in copies:
        copy.wait()

    total = jnp.sum(messages[...], axis=0)
    gram = jnp.concatenate(
        [total] + [pltpu.roll(total, LANES - g * 2 * n, 1) for g in range(1, groups)], 0
    )
    row_id = lax.broadcasted_iota(jnp.int32, gram.shape, 0)
    column_id = lax.broadcasted_iota(jnp.int32, gram.shape, 1)
    off_diagonal = (column_id < n) & (column_id != row_id)
    gram_real = jnp.where(off_diagonal, gram * scale, 0.0)
    gram_imag = jnp.where(off_diagonal, pltpu.roll(gram, LANES - n, 1) * scale, 0.0)

    def along(values, axis):
        return jnp.sum(values, axis=axis, keepdims=True)

    one_real, one_imag = normalize(along(gram_real, 1), along(gram_imag, 1), 0, n)
    row_real, row_imag = normalize(along(gram_real, 0), -along(gram_imag, 0), 1, n)
    rest_real = along(gram_real * row_real - gram_imag * row_imag, 1)
    rest_imag = along(gram_real * row_imag + gram_imag * row_real, 1)
    again_real = one_real * rest_real + one_imag * rest_imag
    again_imag = one_real * rest_imag - one_imag * rest_real
    two_real, two_imag = normalize(again_real, again_imag, 0, n)
    total_real = one_real * two_real - one_imag * two_imag
    total_imag = one_real * two_imag + one_imag * two_real
    mine = lax.broadcasted_iota(jnp.int32, total_real.shape, 0) == me
    own_real = along(jnp.where(mine, total_real, 0.0), 0)
    own_imag = along(jnp.where(mine, total_imag, 0.0), 0)
    correction[...] = jnp.concatenate([own_real, own_imag], 1)
    weights[0] = jnp.broadcast_to(total_real * scale, (n, LANES))
    weights[1] = jnp.broadcast_to(total_imag * scale, (n, LANES))

    step = 4 * OCTET
    for t in range(rows // step):
        span = slice(t * step, (t + 1) * step)
        sum_real = jnp.zeros((step, LANES), F32)
        sum_imag = jnp.zeros((step, LANES), F32)
        for p in range(n):
            weight_real = weights[0, p : p + 1, :]
            weight_imag = weights[1, p : p + 1, :]
            part_real, part_imag = parts[p, 0, span, :], parts[p, 1, span, :]
            sum_real = sum_real + (weight_real * part_real - weight_imag * part_imag)
            sum_imag = sum_imag + (weight_real * part_imag + weight_imag * part_real)
        focused[0, 0, span, :] = sum_real
        focused[1, 0, span, :] = sum_imag


def solution(mesh):
    n = mesh.shape["tile"]

    def per_device(echoes, bin_start, bin_fraction, row_phase, column_phase, row_bin, column_bin):
        samples = echoes.shape[2]
        rows, columns = row_phase.shape[2], column_phase.shape[2]
        first, turn, last = tables(samples)
        bins = samples // LANES
        echo = echoes.reshape(2, bins, LANES)
        fold = fold_table(n)
        vmem = pl.BlockSpec(memory_space=pltpu.VMEM)
        depth = n * 2 * n // LANES
        focused, correction = pl.pallas_call(
            functools.partial(kernel, n),
            out_shape=(
                pltpu.VMEM((2, 1, rows, columns), F32),
                pltpu.VMEM((1, 2), F32),
            ),
            in_specs=[pl.BlockSpec(memory_space=pltpu.SMEM), vmem, pl.BlockSpec(memory_space=pltpu.SMEM)] + [vmem] * 8,
            out_specs=(vmem, vmem),
            scratch_shapes=[
                pltpu.VMEM((2, bins + OCTET, LANES), F32),
                pltpu.VMEM((n, 4, LANES), BF16),
                pltpu.VMEM((n, 4, LANES), BF16),
                pltpu.VMEM((n, rows, 3 * LANES), F32),
                pltpu.VMEM((n, 2, rows, columns), F32),
                pltpu.VMEM((n * 2 * OCTET, rows // OCTET * columns), BF16),
                pltpu.VMEM((depth, LANES), F32),
                pltpu.VMEM((n, depth, LANES), F32),
                pltpu.VMEM((2, n, LANES), F32),
                pltpu.SemaphoreType.DMA((n,)),
                pltpu.SemaphoreType.DMA((n,)),
                pltpu.SemaphoreType.DMA((n,)),
                pltpu.SemaphoreType.DMA((n,)),
            ],
            compiler_params=pltpu.CompilerParams(collective_id=0, has_side_effects=True),
        )(
            bin_start, echo, bin_fraction.T, row_phase, column_phase, row_bin, column_bin,
            jnp.asarray(first), jnp.asarray(turn), jnp.asarray(last), jnp.asarray(fold),
        )
        return focused, correction.T

    split = ("groups", "tile")
    in_specs = (
        P(None, split, None),
        P(split, None),
        P(None, split),
        P(None, split, None),
        P(None, split, None),
        P(None, split, None),
        P(None, split, None),
    )
    out_specs = (P(None, split, None, None), P(None, split))
    return jax.shard_map(per_device, mesh=mesh, in_specs=in_specs, out_specs=out_specs, check_vma=False)
```

```python
import functools
import math

import jax
import jax.numpy as jnp
import numpy as np
from jax import lax
from jax.experimental import pallas as pl
from jax.experimental.pallas import tpu as pltpu
from jax.sharding import PartitionSpec as P

LANES = 128
OCTET = 8
MESH = pl.DeviceIdType.MESH
F32 = jnp.float32
BF16 = jnp.bfloat16


def tables(samples):
    inner = LANES
    outer = samples // inner

    def wave(rows, columns, period):
        product = np.arange(rows)[:, None] * np.arange(columns)[None, :] % period
        phases = product * (2.0 * np.pi / period)
        return np.cos(phases), np.sin(phases)

    def split(table):
        table = table.astype(np.float32)
        high = table.astype(jnp.bfloat16)
        low = (table - high.astype(np.float32)).astype(jnp.bfloat16)
        return np.stack([high, low])

    first = split(np.concatenate(wave(outer, outer, outer), 1))
    last = split(np.concatenate(wave(inner, inner, inner), 1))
    turn = np.stack(wave(outer, inner, samples)) / math.sqrt(samples)
    return first, turn.astype(np.float32), last


def fold_table(pulses):
    block = np.arange(pulses * 2 * OCTET) // OCTET
    pulse, part = block // 2, block % 2
    lane = np.arange(LANES)
    same = [(lane[None, :] == pulse[:, None] + shift * pulses) for shift in (0, 1)]
    real_in = part[:, None] == 0
    real_rows = (same[0] & real_in) * 1.0 + (same[1] & ~real_in) * 1.0
    imag_rows = (same[0] & ~real_in) * 1.0 - (same[1] & real_in) * 1.0
    return np.stack([real_rows, imag_rows]).astype(np.float32)


def dot(a, b, dims=((1,), (0,)), precision=None):
    return lax.dot_general(a, b, (dims, ((), ())), precision=precision, preferred_element_type=F32)


def split3(table_ref, data, dims):
    high = data.astype(BF16)
    low = (data - high.astype(F32)).astype(BF16)
    return dot(table_ref[0], high, dims) + (dot(table_ref[1], high, dims) + dot(table_ref[0], low, dims))


def normalize(real_part, imag_part, axis, count):
    magnitude = real_part * real_part + imag_part * imag_part
    mean = jnp.sum(magnitude, axis=axis, keepdims=True) / count
    denominator = jnp.sqrt(magnitude + mean + 1e-06)
    return real_part / denominator, imag_part / denominator


def kernel(
    n, starts_in, echo_in, first_in, turn_in, last_in, row_phase_in, column_phase_in, row_bin_in, column_bin_in,
    fraction_in, fold_in,
    focused, correction,
    starts, echo, first, turn, last, row_phase, column_phase, row_bin, column_bin, fraction, fold, in_sem,
    spec, outgoing, gathered, steer, parts, gram_in, message, messages, weights,
    send_sem, recv_sem, send_sem2, recv_sem2,
):
    me = lax.axis_index("tile")
    rows = row_phase.shape[2]
    scale = 1.0 / math.sqrt(n)

    barrier = pltpu.get_barrier_semaphore()
    for k in range(1, n):
        pl.semaphore_signal(barrier, inc=1, device_id={"tile": lax.rem(me + k, n)}, device_id_type=MESH)

    sources = (
        starts_in, echo_in, first_in, turn_in, last_in, row_phase_in, column_phase_in, row_bin_in, column_bin_in,
        fraction_in, fold_in,
    )
    targets = (starts, echo, first, turn, last, row_phase, column_phase, row_bin, column_bin, fraction, fold)
    loads = [
        pltpu.make_async_copy(source, target, in_sem.at[i])
        for i, (source, target) in enumerate(zip(sources, targets))
    ]
    for load in loads[1:] + loads[:1]:
        load.start()

    upper = (2 * me) // n

    def other(k):
        place = upper * k + (1 - upper) * (n - 2 - k)
        return place + (place >= me).astype(jnp.int32)


    loads[1].wait()
    loads[2].wait()
    real, imag = echo[0], echo[1]
    data = jnp.concatenate(
        [jnp.concatenate([real, imag], 1), jnp.concatenate([imag, -real], 1)], 0
    )
    section = split3(first, data, ((1,), (0,)))
    half = section.shape[1] // 2
    loads[3].wait()
    loads[4].wait()
    real, imag = section[:, :half], section[:, half:]
    turned_real = real * turn[0] + imag * turn[1]
    turned_imag = imag * turn[0] - real * turn[1]
    data = jnp.concatenate(
        [jnp.concatenate([turned_real, turned_imag], 1), jnp.concatenate([turned_imag, -turned_real], 1)], 0
    )
    spectrum = split3(last, data, ((1,), (1,)))
    bins = spectrum.shape[0]
    spectrum = spectrum.astype(BF16).astype(F32)
    for h in range(2):
        spec[h, 0:bins, :] = spectrum[:, h * LANES : (h + 1) * LANES]
        spec[h, bins:, :] = jnp.zeros((spec.shape[1] - bins, LANES), F32)

    lane = lax.broadcasted_iota(jnp.int32, (OCTET, LANES), 1)
    loads[0].wait()
    for t in range(n):
        start = starts[0, t]
        top = start // LANES
        left = LANES - start % LANES
        pieces = []
        for h in range(2):
            moved = pltpu.roll(spec[h, pl.ds(top, OCTET), :], left % LANES, 1)
            below = pltpu.roll(moved, OCTET - 1, 0)
            pieces.append(jnp.where(lane < left, moved, below)[0:2])
        outgoing[t] = jnp.concatenate(pieces, 0).astype(BF16)

    pl.semaphore_wait(barrier, n - 1)

    def window_copy(device, slot):
        return pltpu.make_async_remote_copy(
            src_ref=outgoing.at[device],
            dst_ref=gathered.at[slot],
            send_sem=send_sem.at[device],
            recv_sem=recv_sem.at[slot],
            device_id={"tile": device},
            device_id_type=MESH,
        )

    for k in range(n - 1):
        window_copy(other(k), me).start()
    gathered[me] = outgoing[me]

    def rounded(values):
        return values.astype(BF16).astype(F32)

    for load in loads[5:]:
        load.wait()
    angles = row_phase[:, 0, :]
    left_side = jnp.concatenate(
        [
            rounded(jnp.cos(angles)),
            rounded(jnp.sin(angles)),
            row_bin[:, 0, :].astype(F32),
            jnp.ones((n, rows), F32),
        ],
        0,
    )
    left_side = left_side.T.astype(BF16)
    angles = column_phase[:, 0, :]
    cosine, sine = rounded(jnp.cos(angles)), rounded(jnp.sin(angles))
    zero, one = jnp.zeros((n, LANES), F32), jnp.ones((n, LANES), F32)
    right_side = jnp.concatenate(
        [
            jnp.concatenate([cosine, sine, zero], 1),
            jnp.concatenate([-sine, cosine, zero], 1),
            jnp.concatenate([zero, zero, one], 1),
            jnp.concatenate([zero, zero, column_bin[:, 0, :].astype(F32)], 1),
        ],
        0,
    )
    owner = lax.rem(lax.broadcasted_iota(jnp.int32, right_side.shape, 0), n)
    for p in range(n):
        steer[p] = dot(left_side, jnp.where(owner == p, right_side, 0.0).astype(BF16))

    lane4 = lax.broadcasted_iota(jnp.int32, (4, LANES), 1)

    def contribute(p):
        window = gathered[p].astype(F32)
        moved = pltpu.roll(window, LANES - 1, 1)
        below = jnp.concatenate([moved[1:4], moved[0:1]], 0)
        shifted = jnp.where(lane4 == LANES - 1, below, moved)
        share = fraction[0, p]
        profile = ((1.0 - share) * window + share * shifted).astype(BF16).astype(F32)
        index = steer[p, :, 2 * LANES :].astype(jnp.int32)
        low = index < LANES
        index = index & (LANES - 1)

        def pick(row):
            source = jnp.broadcast_to(profile[row : row + 1, :], (rows, LANES))
            return jnp.take_along_axis(source, index, axis=1, mode="promise_in_bounds")

        real = jnp.where(low, pick(0), pick(1))
        imag = jnp.where(low, pick(2), pick(3))
        turn_real, turn_imag = steer[p, :, :LANES], steer[p, :, LANES : 2 * LANES]
        part_real = turn_real * real - turn_imag * imag
        part_imag = turn_real * imag + turn_imag * real
        parts[p, 0] = part_real
        parts[p, 1] = part_imag
        own_rows = pl.ds(pl.multiple_of(p * 2 * OCTET, 2 * OCTET), 2 * OCTET)
        for t in range(rows // OCTET):
            pair = jnp.concatenate(
                [part_real[t * OCTET : (t + 1) * OCTET], part_imag[t * OCTET : (t + 1) * OCTET]], 0
            )
            gram_in[own_rows, t * LANES : (t + 1) * LANES] = pair.astype(BF16)

    contribute(me)
    near_first = [other(k) for k in reversed(range(n - 1))]
    cuts = [0, n // 2 - 1, 3 * n // 4 - 1, n - 1]
    for begin, end in zip(cuts[:-1], cuts[1:]):
        for device in near_first[begin:end]:
            window_copy(device, device).wait()
        for device in near_first[begin:end]:
            contribute(device)

    values = gram_in[...]
    product = dot(values, values, ((1,), (1,)))
    row_id = lax.broadcasted_iota(jnp.int32, product.shape, 0)
    column_id = lax.broadcasted_iota(jnp.int32, product.shape, 1)
    product = jnp.where(lax.rem(row_id, OCTET) == lax.rem(column_id, OCTET), product, 0.0)
    product = product.reshape(n, 2, OCTET, product.shape[1])
    gram = dot(jnp.sum(product[:, 0], axis=1), fold[0], precision=lax.Precision.HIGHEST)
    gram = gram + dot(jnp.sum(product[:, 1], axis=1), fold[1], precision=lax.Precision.HIGHEST)
    groups = LANES // (2 * n)
    depth = n // groups
    packed = gram[0:depth]
    for g in range(1, groups):
        packed = packed + pltpu.roll(gram[g * depth : (g + 1) * depth], g * 2 * n, 1)
    message[...] = packed
    messages[me] = packed

    def gram_copy(device, slot):
        return pltpu.make_async_remote_copy(
            src_ref=message,
            dst_ref=messages.at[slot],
            send_sem=send_sem2.at[device],
            recv_sem=recv_sem2.at[slot],
            device_id={"tile": device},
            device_id_type=MESH,
        )

    for k in range(n - 1):
        gram_copy(other(k), me).start()
    for device in near_first:
        gram_copy(device, device).wait()

    total = jnp.sum(messages[...], axis=0)
    gram = jnp.concatenate(
        [total] + [pltpu.roll(total, LANES - g * 2 * n, 1) for g in range(1, groups)], 0
    )
    row_id = lax.broadcasted_iota(jnp.int32, gram.shape, 0)
    column_id = lax.broadcasted_iota(jnp.int32, gram.shape, 1)
    off_diagonal = (column_id < n) & (column_id != row_id)
    gram_real = jnp.where(off_diagonal, gram * scale, 0.0)
    gram_imag = jnp.where(off_diagonal, pltpu.roll(gram, LANES - n, 1) * scale, 0.0)

    def along(values, axis):
        return jnp.sum(values, axis=axis, keepdims=True)

    one_real, one_imag = normalize(along(gram_real, 1), along(gram_imag, 1), 0, n)
    row_real, row_imag = normalize(along(gram_real, 0), -along(gram_imag, 0), 1, n)
    rest_real = along(gram_real * row_real - gram_imag * row_imag, 1)
    rest_imag = along(gram_real * row_imag + gram_imag * row_real, 1)
    again_real = one_real * rest_real + one_imag * rest_imag
    again_imag = one_real * rest_imag - one_imag * rest_real
    two_real, two_imag = normalize(again_real, again_imag, 0, n)
    total_real = one_real * two_real - one_imag * two_imag
    total_imag = one_real * two_imag + one_imag * two_real
    mine = lax.broadcasted_iota(jnp.int32, total_real.shape, 0) == me
    own_real = along(jnp.where(mine, total_real, 0.0), 0)
    own_imag = along(jnp.where(mine, total_imag, 0.0), 0)
    correction[...] = jnp.concatenate([own_real, own_imag], 1)
    weights[0] = jnp.broadcast_to(total_real * scale, (n, LANES))
    weights[1] = jnp.broadcast_to(total_imag * scale, (n, LANES))

    step = 4 * OCTET
    for t in range(rows // step):
        span = slice(t * step, (t + 1) * step)
        sum_real = jnp.zeros((step, LANES), F32)
        sum_imag = jnp.zeros((step, LANES), F32)
        for p in range(n):
            weight_real = weights[0, p : p + 1, :]
            weight_imag = weights[1, p : p + 1, :]
            part_real, part_imag = parts[p, 0, span, :], parts[p, 1, span, :]
            sum_real = sum_real + (weight_real * part_real - weight_imag * part_imag)
            sum_imag = sum_imag + (weight_real * part_imag + weight_imag * part_real)
        focused[0, 0, span, :] = sum_real
        focused[1, 0, span, :] = sum_imag


def solution(mesh):
    n = mesh.shape["tile"]

    def per_device(echoes, bin_start, bin_fraction, row_phase, column_phase, row_bin, column_bin):
        samples = echoes.shape[2]
        rows, columns = row_phase.shape[2], column_phase.shape[2]
        first, turn, last = tables(samples)
        bins = samples // LANES
        echo = echoes.reshape(2, bins, LANES)
        fold = fold_table(n)
        vmem = pl.BlockSpec(memory_space=pltpu.VMEM)
        operands = (
            bin_start, echo, jnp.asarray(first), jnp.asarray(turn), jnp.asarray(last),
            row_phase, column_phase, row_bin, column_bin, bin_fraction.T, jnp.asarray(fold),
        )
        depth = n * 2 * n // LANES
        focused, correction = pl.pallas_call(
            functools.partial(kernel, n),
            out_shape=(
                pltpu.VMEM((2, 1, rows, columns), F32),
                pltpu.VMEM((1, 2), F32),
            ),
            in_specs=[pl.BlockSpec(memory_space=pltpu.HBM)] * len(operands),
            out_specs=(vmem, vmem),
            scratch_shapes=[pltpu.SMEM(bin_start.shape, jnp.int32)]
            + [pltpu.VMEM(operand.shape, operand.dtype) for operand in operands[1:9]]
            + [pltpu.SMEM((1, n), F32), pltpu.VMEM(fold.shape, F32), pltpu.SemaphoreType.DMA((len(operands),))]
            + [
                pltpu.VMEM((2, bins + OCTET, LANES), F32),
                pltpu.VMEM((n, 4, LANES), BF16),
                pltpu.VMEM((n, 4, LANES), BF16),
                pltpu.VMEM((n, rows, 3 * LANES), F32),
                pltpu.VMEM((n, 2, rows, columns), F32),
                pltpu.VMEM((n * 2 * OCTET, rows // OCTET * columns), BF16),
                pltpu.VMEM((depth, LANES), F32),
                pltpu.VMEM((n, depth, LANES), F32),
                pltpu.VMEM((2, n, LANES), F32),
                pltpu.SemaphoreType.DMA((n,)),
                pltpu.SemaphoreType.DMA((n,)),
                pltpu.SemaphoreType.DMA((n,)),
                pltpu.SemaphoreType.DMA((n,)),
            ],
            compiler_params=pltpu.CompilerParams(collective_id=0, has_side_effects=True),
        )(*operands)
        return focused, correction.T

    split = ("groups", "tile")
    in_specs = (
        P(None, split, None),
        P(split, None),
        P(None, split),
        P(None, split, None),
        P(None, split, None),
        P(None, split, None),
        P(None, split, None),
    )
    out_specs = (P(None, split, None, None), P(None, split))
    return jax.shard_map(per_device, mesh=mesh, in_specs=in_specs, out_specs=out_specs, check_vma=False)
```

```python
import functools
import math

import jax
import jax.numpy as jnp
import numpy as np
from jax import lax
from jax.experimental import pallas as pl
from jax.experimental.pallas import tpu as pltpu
from jax.sharding import PartitionSpec as P

LANES = 128
OCTET = 8
MESH = pl.DeviceIdType.MESH
F32 = jnp.float32
BF16 = jnp.bfloat16


def tables(samples):
    inner = LANES
    outer = samples // inner

    def wave(rows, columns, period):
        product = np.arange(rows)[:, None] * np.arange(columns)[None, :] % period
        phases = product * (2.0 * np.pi / period)
        return np.cos(phases), np.sin(phases)

    def split(table):
        table = table.astype(np.float32)
        high = table.astype(jnp.bfloat16)
        low = (table - high.astype(np.float32)).astype(jnp.bfloat16)
        return np.stack([high, low])

    first = split(np.concatenate(wave(outer, outer, outer), 1))
    last = split(np.concatenate(wave(inner, inner, inner), 1))
    turn = np.stack(wave(outer, inner, samples)) / math.sqrt(samples)
    return first, turn.astype(np.float32), last


def fold_table(pulses):
    block = np.arange(pulses * 2 * OCTET) // OCTET
    pulse, part = block // 2, block % 2
    lane = np.arange(LANES)
    same = [(lane[None, :] == pulse[:, None] + shift * pulses) for shift in (0, 1)]
    real_in = part[:, None] == 0
    real_rows = (same[0] & real_in) * 1.0 + (same[1] & ~real_in) * 1.0
    imag_rows = (same[0] & ~real_in) * 1.0 - (same[1] & real_in) * 1.0
    return np.stack([real_rows, imag_rows]).astype(np.float32)


def dot(a, b, dims=((1,), (0,)), precision=None):
    return lax.dot_general(a, b, (dims, ((), ())), precision=precision, preferred_element_type=F32)


def split3(table_ref, data, dims):
    high = data.astype(BF16)
    low = (data - high.astype(F32)).astype(BF16)
    return dot(table_ref[0], high, dims) + (dot(table_ref[1], high, dims) + dot(table_ref[0], low, dims))


def normalize(real_part, imag_part, axis, count):
    magnitude = real_part * real_part + imag_part * imag_part
    mean = jnp.sum(magnitude, axis=axis, keepdims=True) / count
    denominator = jnp.sqrt(magnitude + mean + 1e-06)
    return real_part / denominator, imag_part / denominator


def kernel(
    n, starts_in, echo_in, first_in, turn_in, last_in, row_phase_in, column_phase_in, row_bin_in, column_bin_in,
    fraction_in, fold_in,
    parts, weights, correction,
    starts, echo, first, turn, last, row_phase, column_phase, row_bin, column_bin, fraction, fold, in_sem,
    spec, outgoing, gathered, steer, gram_in, message, messages,
    send_sem, recv_sem, send_sem2, recv_sem2,
):
    me = lax.axis_index("tile")
    rows = row_phase.shape[2]
    scale = 1.0 / math.sqrt(n)

    barrier = pltpu.get_barrier_semaphore()
    for k in range(1, n):
        pl.semaphore_signal(barrier, inc=1, device_id={"tile": lax.rem(me + k, n)}, device_id_type=MESH)

    sources = (
        starts_in, echo_in, first_in, turn_in, last_in, row_phase_in, column_phase_in, row_bin_in, column_bin_in,
        fraction_in, fold_in,
    )
    targets = (starts, echo, first, turn, last, row_phase, column_phase, row_bin, column_bin, fraction, fold)
    loads = [
        pltpu.make_async_copy(source, target, in_sem.at[i])
        for i, (source, target) in enumerate(zip(sources, targets))
    ]
    for load in loads[1:] + loads[:1]:
        load.start()

    block = math.gcd(n, 4)
    here, upper = me // block, (2 * me) // n

    def within(i):
        place = 0
        for bit in (1, 2):
            if bit < block:
                place = place + lax.rem(lax.rem(me // bit, 2) + (i // bit) % 2, 2) * bit
        return place

    near_first = [here * block + within(i) for i in range(1, block)]
    for k in range(n // block - 1):
        place = upper * (n // block - 2 - k) + (1 - upper) * k
        place = place + (place >= here).astype(jnp.int32)
        near_first += [place * block + within(i) for i in range(block)]
    far_first = near_first[::-1]

    loads[1].wait()
    loads[2].wait()
    real, imag = echo[0], echo[1]
    data = jnp.concatenate(
        [jnp.concatenate([real, imag], 1), jnp.concatenate([imag, -real], 1)], 0
    )
    section = split3(first, data, ((1,), (0,)))
    half = section.shape[1] // 2
    loads[3].wait()
    loads[4].wait()
    real, imag = section[:, :half], section[:, half:]
    turned_real = real * turn[0] + imag * turn[1]
    turned_imag = imag * turn[0] - real * turn[1]
    data = jnp.concatenate(
        [jnp.concatenate([turned_real, turned_imag], 1), jnp.concatenate([turned_imag, -turned_real], 1)], 0
    )
    spectrum = split3(last, data, ((1,), (1,)))
    bins = spectrum.shape[0]
    spectrum = spectrum.astype(BF16).astype(F32)
    for h in range(2):
        spec[h, 0:bins, :] = spectrum[:, h * LANES : (h + 1) * LANES]
        spec[h, bins:, :] = jnp.zeros((spec.shape[1] - bins, LANES), F32)

    lane = lax.broadcasted_iota(jnp.int32, (OCTET, LANES), 1)
    loads[0].wait()
    for t in range(n):
        start = starts[0, t]
        top = start // LANES
        left = LANES - start % LANES
        pieces = []
        for h in range(2):
            moved = pltpu.roll(spec[h, pl.ds(top, OCTET), :], left % LANES, 1)
            below = pltpu.roll(moved, OCTET - 1, 0)
            pieces.append(jnp.where(lane < left, moved, below)[0:2])
        outgoing[t] = jnp.concatenate(pieces, 0).astype(BF16)

    pl.semaphore_wait(barrier, n - 1)

    def window_copy(device, slot):
        return pltpu.make_async_remote_copy(
            src_ref=outgoing.at[device],
            dst_ref=gathered.at[slot],
            send_sem=send_sem.at[device],
            recv_sem=recv_sem.at[slot],
            device_id={"tile": device},
            device_id_type=MESH,
        )

    for device in far_first:
        window_copy(device, me).start()
    gathered[me] = outgoing[me]

    def rounded(values):
        return values.astype(BF16).astype(F32)

    for load in loads[5:]:
        load.wait()
    angles = row_phase[:, 0, :]
    left_side = jnp.concatenate(
        [
            rounded(jnp.cos(angles)),
            rounded(jnp.sin(angles)),
            row_bin[:, 0, :].astype(F32),
            jnp.ones((n, rows), F32),
        ],
        0,
    )
    left_side = left_side.T.astype(BF16)
    angles = column_phase[:, 0, :]
    cosine, sine = rounded(jnp.cos(angles)), rounded(jnp.sin(angles))
    zero, one = jnp.zeros((n, LANES), F32), jnp.ones((n, LANES), F32)
    right_side = jnp.concatenate(
        [
            jnp.concatenate([cosine, sine, zero], 1),
            jnp.concatenate([-sine, cosine, zero], 1),
            jnp.concatenate([zero, zero, one], 1),
            jnp.concatenate([zero, zero, column_bin[:, 0, :].astype(F32)], 1),
        ],
        0,
    )
    owner = lax.rem(lax.broadcasted_iota(jnp.int32, right_side.shape, 0), n)
    for p in range(n):
        steer[p] = dot(left_side, jnp.where(owner == p, right_side, 0.0).astype(BF16))

    lane4 = lax.broadcasted_iota(jnp.int32, (4, LANES), 1)

    def contribute(p):
        window = gathered[p].astype(F32)
        moved = pltpu.roll(window, LANES - 1, 1)
        below = jnp.concatenate([moved[1:4], moved[0:1]], 0)
        shifted = jnp.where(lane4 == LANES - 1, below, moved)
        share = fraction[0, p]
        profile = ((1.0 - share) * window + share * shifted).astype(BF16).astype(F32)
        index = steer[p, :, 2 * LANES :].astype(jnp.int32)
        low = index < LANES
        index = index & (LANES - 1)

        def pick(row):
            source = jnp.broadcast_to(profile[row : row + 1, :], (rows, LANES))
            return jnp.take_along_axis(source, index, axis=1, mode="promise_in_bounds")

        real = jnp.where(low, pick(0), pick(1))
        imag = jnp.where(low, pick(2), pick(3))
        turn_real, turn_imag = steer[p, :, :LANES], steer[p, :, LANES : 2 * LANES]
        part_real = turn_real * real - turn_imag * imag
        part_imag = turn_real * imag + turn_imag * real
        parts[p, 0] = part_real
        parts[p, 1] = part_imag
        own_rows = pl.ds(pl.multiple_of(p * 2 * OCTET, 2 * OCTET), 2 * OCTET)
        for t in range(rows // OCTET):
            pair = jnp.concatenate(
                [part_real[t * OCTET : (t + 1) * OCTET], part_imag[t * OCTET : (t + 1) * OCTET]], 0
            )
            gram_in[own_rows, t * LANES : (t + 1) * LANES] = pair.astype(BF16)

    contribute(me)
    cuts = [0, n // 2 - 1, n - 5, n - 3, n - 1]
    for begin, end in zip(cuts[:-1], cuts[1:]):
        for device in near_first[begin:end]:
            window_copy(device, device).wait()
        for device in near_first[begin:end]:
            contribute(device)

    values = gram_in[...]
    product = dot(values, values, ((1,), (1,)))
    row_id = lax.broadcasted_iota(jnp.int32, product.shape, 0)
    column_id = lax.broadcasted_iota(jnp.int32, product.shape, 1)
    product = jnp.where(lax.rem(row_id, OCTET) == lax.rem(column_id, OCTET), product, 0.0)
    product = product.reshape(n, 2, OCTET, product.shape[1])
    gram = dot(jnp.sum(product[:, 0], axis=1), fold[0], precision=lax.Precision.HIGHEST)
    gram = gram + dot(jnp.sum(product[:, 1], axis=1), fold[1], precision=lax.Precision.HIGHEST)
    groups = LANES // (2 * n)
    depth = n // groups
    packed = gram[0:depth]
    for g in range(1, groups):
        packed = packed + pltpu.roll(gram[g * depth : (g + 1) * depth], g * 2 * n, 1)
    message[...] = packed
    messages[me] = packed

    def gram_copy(device, slot):
        return pltpu.make_async_remote_copy(
            src_ref=message,
            dst_ref=messages.at[slot],
            send_sem=send_sem2.at[device],
            recv_sem=recv_sem2.at[slot],
            device_id={"tile": device},
            device_id_type=MESH,
        )

    for device in far_first:
        gram_copy(device, me).start()
    for device in near_first:
        gram_copy(device, device).wait()

    total = jnp.sum(messages[...], axis=0)
    gram = jnp.concatenate(
        [total] + [pltpu.roll(total, LANES - g * 2 * n, 1) for g in range(1, groups)], 0
    )
    row_id = lax.broadcasted_iota(jnp.int32, gram.shape, 0)
    column_id = lax.broadcasted_iota(jnp.int32, gram.shape, 1)
    off_diagonal = (column_id < n) & (column_id != row_id)
    gram_real = jnp.where(off_diagonal, gram * scale, 0.0)
    gram_imag = jnp.where(off_diagonal, pltpu.roll(gram, LANES - n, 1) * scale, 0.0)

    def along(values, axis):
        return jnp.sum(values, axis=axis, keepdims=True)

    one_real, one_imag = normalize(along(gram_real, 1), along(gram_imag, 1), 0, n)
    row_real, row_imag = normalize(along(gram_real, 0), -along(gram_imag, 0), 1, n)
    rest_real = along(gram_real * row_real - gram_imag * row_imag, 1)
    rest_imag = along(gram_real * row_imag + gram_imag * row_real, 1)
    again_real = one_real * rest_real + one_imag * rest_imag
    again_imag = one_real * rest_imag - one_imag * rest_real
    two_real, two_imag = normalize(again_real, again_imag, 0, n)
    total_real = one_real * two_real - one_imag * two_imag
    total_imag = one_real * two_imag + one_imag * two_real
    mine = lax.broadcasted_iota(jnp.int32, total_real.shape, 0) == me
    own_real = along(jnp.where(mine, total_real, 0.0), 0)
    own_imag = along(jnp.where(mine, total_imag, 0.0), 0)
    correction[...] = jnp.concatenate([own_real, own_imag], 1)
    weights[0] = jnp.broadcast_to(total_real * scale, (n, LANES))
    weights[1] = jnp.broadcast_to(total_imag * scale, (n, LANES))


def finish(parts, weights, own, focused, correction, image, sem):
    n, rows = parts.shape[0], parts.shape[2]
    step = 4 * OCTET
    stores = [pltpu.make_async_copy(own, correction, sem.at[0])]
    stores[0].start()
    for t in range(rows // step):
        span = pl.ds(t * step, step)
        sum_real = jnp.zeros((step, LANES), F32)
        sum_imag = jnp.zeros((step, LANES), F32)
        for p in range(n):
            weight_real = weights[0, p : p + 1, :]
            weight_imag = weights[1, p : p + 1, :]
            part_real, part_imag = parts[p, 0, span, :], parts[p, 1, span, :]
            sum_real = sum_real + (weight_real * part_real - weight_imag * part_imag)
            sum_imag = sum_imag + (weight_real * part_imag + weight_imag * part_real)
        image[0, 0, span, :] = sum_real
        image[1, 0, span, :] = sum_imag
        stores.append(
            pltpu.make_async_copy(image.at[:, :, span, :], focused.at[:, :, span, :], sem.at[t + 1])
        )
        stores[-1].start()
    for store in stores:
        store.wait()


def solution(mesh):
    n = mesh.shape["tile"]

    def per_device(echoes, bin_start, bin_fraction, row_phase, column_phase, row_bin, column_bin):
        samples = echoes.shape[2]
        rows, columns = row_phase.shape[2], column_phase.shape[2]
        first, turn, last = tables(samples)
        bins = samples // LANES
        echo = echoes.reshape(2, bins, LANES)
        fold = fold_table(n)
        vmem = pl.BlockSpec(memory_space=pltpu.VMEM)
        operands = (
            bin_start, echo, jnp.asarray(first), jnp.asarray(turn), jnp.asarray(last),
            row_phase, column_phase, row_bin, column_bin, bin_fraction.T, jnp.asarray(fold),
        )
        depth = n * 2 * n // LANES
        parts, weights, own = pl.pallas_call(
            functools.partial(kernel, n),
            out_shape=(
                pltpu.VMEM((n, 2, rows, columns), F32),
                pltpu.VMEM((2, n, LANES), F32),
                pltpu.VMEM((1, 2), F32),
            ),
            in_specs=[pl.BlockSpec(memory_space=pltpu.HBM)] * len(operands),
            out_specs=(vmem, vmem, vmem),
            scratch_shapes=[pltpu.SMEM(bin_start.shape, jnp.int32)]
            + [pltpu.VMEM(operand.shape, operand.dtype) for operand in operands[1:9]]
            + [pltpu.SMEM((1, n), F32), pltpu.VMEM(fold.shape, F32), pltpu.SemaphoreType.DMA((len(operands),))]
            + [
                pltpu.VMEM((2, bins + OCTET, LANES), F32),
                pltpu.VMEM((n, 4, LANES), BF16),
                pltpu.VMEM((n, 4, LANES), BF16),
                pltpu.VMEM((n, rows, 3 * LANES), F32),
                pltpu.VMEM((n * 2 * OCTET, rows // OCTET * columns), BF16),
                pltpu.VMEM((depth, LANES), F32),
                pltpu.VMEM((n, depth, LANES), F32),
                pltpu.SemaphoreType.DMA((n,)),
                pltpu.SemaphoreType.DMA((n,)),
                pltpu.SemaphoreType.DMA((n,)),
                pltpu.SemaphoreType.DMA((n,)),
            ],
            compiler_params=pltpu.CompilerParams(
                collective_id=0, has_side_effects=True, vmem_limit_bytes=32 << 20
            ),
        )(*operands)
        focused, correction = pl.pallas_call(
            finish,
            out_shape=(
                jax.ShapeDtypeStruct((2, 1, rows, columns), F32),
                jax.ShapeDtypeStruct((1, 2), F32),
            ),
            in_specs=[vmem] * 3,
            out_specs=[pl.BlockSpec(memory_space=pltpu.HBM)] * 2,
            scratch_shapes=[
                pltpu.VMEM((2, 1, rows, columns), F32),
                pltpu.SemaphoreType.DMA((rows // (4 * OCTET) + 1,)),
            ],
            compiler_params=pltpu.CompilerParams(vmem_limit_bytes=16 << 20),
        )(*[pltpu.with_memory_space_constraint(value, pltpu.VMEM) for value in (parts, weights, own)])
        return focused, correction.T

    split = ("groups", "tile")
    in_specs = (
        P(None, split, None),
        P(split, None),
        P(None, split),
        P(None, split, None),
        P(None, split, None),
        P(None, split, None),
        P(None, split, None),
    )
    out_specs = (P(None, split, None, None), P(None, split))
    return jax.shard_map(per_device, mesh=mesh, in_specs=in_specs, out_specs=out_specs, check_vma=False)
```
